32 devices in a mesh: row: 8 (over y, x, core), col: 4 (over z).
Axes of the slice: x: 2, y: 2, z: 4, core: 2. Of those that a mesh axis runs over, the one named last changes fastest.
Arguments:
- queries: bfloat16 [256, 32, 128], P(('row', 'col')), may hold values from -1 to 1
- documents: bfloat16 [256, 128, 128], P(('row', 'col')), may hold values from -1 to 1
- lengths: int32 [256], P(('row', 'col')), may hold values from 1 to 128
- positives: int32 [256], P(('row', 'col')), may hold values from 0 to 255
Outputs:
- query_loss: float32 [256], P(('row', 'col'))
The draws below stay inside these ranges and needn't reach their ends.
All inputs are finite; a program needn't handle non-finite values.
Results may differ from the reference program's by a relative error of at most 0.0003.
Values may be sent and summed in bfloat16 or wider, within the bound.
A program may use at most 64 MiB of HBM per device.

```python
import jax
import jax.numpy as jnp
from jax import lax

DIM = 128
QT = 32
DT = 128
NQ = 256
ND = 256


def draw_queries(key, part):
    own_key = jax.random.fold_in(key, 71)
    spread = 0.8 * DIM ** (-0.5)
    values = jnp.clip(spread * jax.random.normal(own_key, (NQ, QT, DIM), jnp.float32), -1.0, 1.0)
    return values.astype(jnp.bfloat16)


def draw_documents(key, part):
    own_key = jax.random.fold_in(key, 72)
    spread = 0.8 * DIM ** (-0.5)
    values = jnp.clip(spread * jax.random.normal(own_key, (ND, DT, DIM), jnp.float32), -1.0, 1.0)
    return values.astype(jnp.bfloat16)


def with_ends(array, stream_key, smallest, high):
    longest = array.shape.index(max(array.shape))
    spots = []
    for shift in (0, 1):
        where = [jax.random.randint(jax.random.fold_in(stream_key, axis), (), 0, length) for axis, length in enumerate(array.shape)]
        where[longest] = (where[longest] + shift) % array.shape[longest]
        spots.append(tuple(where))
    return array.at[spots[0]].set(smallest).at[spots[1]].set(high)


def setup_inputs(seed: int = 0) -> dict:
    key_list = jax.random.split(jax.random.key(seed), 5)
    return {
        "queries": draw_queries(jax.random.fold_in(key_list[4], 71), 0),
        "documents": draw_documents(jax.random.fold_in(key_list[4], 71), 0),
        "lengths": with_ends(jax.random.randint(key_list[2], (ND,), 1, DT + 1), jax.random.fold_in(key_list[2], 1), 1, DT).astype(jnp.int32),
        "positives": with_ends(jax.random.randint(key_list[3], (NQ,), 0, ND), jax.random.fold_in(key_list[3], 1), 0, ND - 1).astype(jnp.int32),
    }


neg_fill = -1.0e30


def reference(queries, documents, lengths, positives):
    query_flat = queries.astype(jnp.float32).reshape(NQ * QT, DIM)
    token_slots = jnp.arange(DT, dtype=jnp.int32)

    def one_document(doc_pair):
        document, doc_length = doc_pair
        similar = lax.dot_general(query_flat, document.astype(jnp.float32), (((1,), (1,)), ((), ())), precision=lax.Precision.HIGHEST, preferred_element_type=jnp.float32)
        similar = jnp.where(token_slots[None, :] < doc_length, similar, neg_fill)
        return jnp.sum(jnp.max(similar, axis=1).reshape(NQ, QT), axis=1)

    scores = lax.map(one_document, (documents, lengths)).T
    peak_score = jnp.max(scores, axis=1, keepdims=True)
    log_total = peak_score[:, 0] + jnp.log(jnp.sum(jnp.exp(scores - peak_score), axis=1))
    doc_ids = jnp.arange(ND, dtype=jnp.int32)
    positive_score = jnp.sum(jnp.where(doc_ids[None, :] == positives[:, None], scores, 0.0), axis=1)
    return log_total - positive_score
```

```python
import functools

import jax
import jax.numpy as jnp
from jax import lax
from jax.experimental import pallas as pl
from jax.experimental.pallas import tpu as pltpu
from jax.sharding import PartitionSpec as P

MESH = pl.DeviceIdType.MESH
QUAD = 4
PARTS = 4


def kernel(
    Y, C, per, QT, DT,
    len_ref, pos_ref, q_ref, d_ref, out_ref,
    dbuf, qbuf, best, ones, sc_out, sc_in,
    d_send, d_recv, x_send, x_recv, r_send, r_recv, q_send, q_recv, s_send, s_recv,
):
    row, z = lax.axis_index("row"), lax.axis_index("col")
    y, k = row // QUAD, row % QUAD
    core, side = k % 2, k // 2
    core_peer = (row + 1 - 2 * core, z)
    chip_peer = (row + 2 - 4 * side, z)
    G = Y * C
    rows = per * DT
    toks = per * QT
    part = rows // PARTS

    def place(dy, dz):
        return (((y + dy) % Y) * QUAD + k, (z + dz) % C)

    def slot(dy, dz):
        return (dy % Y) * C + dz % C

    barrier = pltpu.get_barrier_semaphore()
    peers = [core_peer, chip_peer]
    peers += [place(0, d) for d in range(1, C)] + [place(e, 0) for e in range(1, Y)]
    for peer in peers:
        pl.semaphore_signal(barrier, inc=1, device_id=peer, device_id_type=MESH)

    slots = lax.broadcasted_iota(jnp.int32, (DT, d_ref.shape[1]), 0)
    for i in range(per):
        block = d_ref[i * DT:(i + 1) * DT, :].astype(jnp.float32)
        block = jnp.where(slots < len_ref[i], block, block[0:1, :])
        dbuf[0, i * DT:(i + 1) * DT, :] = block.astype(jnp.bfloat16)
    qbuf[0] = q_ref[...]
    lane = lax.broadcasted_iota(jnp.int32, ones.shape, 1)
    tok = lax.broadcasted_iota(jnp.int32, ones.shape, 0)
    ones[...] = jnp.where(lane % (QUAD * per) == tok // QT, 1.0, 0.0).astype(jnp.bfloat16)

    pl.semaphore_wait(barrier, len(peers))

    def copy(src, dst, send, recv, peer):
        return pltpu.make_async_remote_copy(
            src_ref=src, dst_ref=dst, send_sem=send, recv_sem=recv,
            device_id=peer, device_id_type=MESH,
        )

    def piece(b, i):
        return dbuf.at[b, pl.ds(i * part, part), :]

    started = []

    def go(c):
        c.start()
        started.append(c)
        return c

    got_q = {}
    for d in range(1, C):
        s = slot(0, -d)
        got_q[s] = go(copy(q_ref, qbuf.at[s], q_send.at[s], q_recv.at[s], place(0, d)))
    for e in range(1, Y):
        s = slot(-e, 0)
        got_q[s] = go(copy(q_ref, qbuf.at[s], q_send.at[s], q_recv.at[s], place(e, 0)))
    got_x = [
        go(copy(piece(0, i), piece(2, i), x_send.at[i], x_recv.at[i], chip_peer))
        for i in range(PARTS)
    ]
    got_d = go(copy(dbuf.at[0], dbuf.at[1], d_send, d_recv, core_peer))
    got_r = []

    def unit(s, b):
        sim = lax.dot_general(
            dbuf[b], qbuf[s], (((1,), (1,)), ((), ())), preferred_element_type=jnp.float32
        )
        top = jnp.max(sim.reshape(per, DT, toks), axis=1)
        best[s * per:(s + 1) * per, b * toks:(b + 1) * toks] = top

    unit(0, 0)
    got_d.wait_recv()
    unit(0, 1)
    near = [0]
    for i in range(max(PARTS, C - 1)):
        if i < PARTS:
            got_x[i].wait_recv()
            got_r.append(go(copy(piece(2, i), piece(3, i), r_send.at[i], r_recv.at[i], core_peer)))
        if i < C - 1:
            s = slot(0, -(i + 1))
            got_q[s].wait_recv()
            for e in range(1, Y):
                t = slot(-e, -(i + 1))
                got_q[t] = go(copy(qbuf.at[s], qbuf.at[t], q_send.at[t], q_recv.at[t], place(e, 0)))
            unit(s, 0)
            unit(s, 1)
            near.append(s)
    for e in range(1, Y):
        s = slot(-e, 0)
        got_q[s].wait_recv()
        unit(s, 0)
        unit(s, 1)
        near.append(s)
    for s in near:
        unit(s, 2)
    for c in got_r:
        c.wait_recv()
    for s in near:
        unit(s, 3)
    for i in range(C - 1):
        for e in range(1, Y):
            s = slot(-e, -(i + 1))
            got_q[s].wait_recv()
            for b in range(QUAD):
                unit(s, b)

    x = best[...]
    hi = x.astype(jnp.bfloat16)
    x = x - hi.astype(jnp.float32)
    mid = x.astype(jnp.bfloat16)
    low = (x - mid.astype(jnp.float32)).astype(jnp.bfloat16)
    sums = jnp.dot(low, ones[...], preferred_element_type=jnp.float32)
    sums += jnp.dot(mid, ones[...], preferred_element_type=jnp.float32)
    sums += jnp.dot(hi, ones[...], preferred_element_type=jnp.float32)
    sums = sums.reshape(G, per, sums.shape[1])
    sc_out[...] = sums
    sc_in[0] = sums[0]
    got_s = []
    for dy in range(Y):
        for dz in range(C):
            if dy or dz:
                s, t = slot(dy, dz), slot(-dy, -dz)
                got_s.append(go(copy(
                    sc_out.at[s], sc_in.at[t], s_send.at[t], s_recv.at[t], place(dy, dz)
                )))
    for c in got_s:
        c.wait_recv()

    def total(op, tiles):
        t = tiles[0]
        for g in range(1, G):
            t = op(t, tiles[g])
        shift = 1
        while shift < per:
            t = op(t, pltpu.roll(t, shift, 0))
            shift *= 2
        shift = per
        while shift < QUAD * per:
            t = op(t, pltpu.roll(t, shift, 1))
            shift *= 2
        return t

    tile = sc_in.shape[1:]
    lane = lax.broadcasted_iota(jnp.int32, tile, 1)
    doc = lax.broadcasted_iota(jnp.int32, tile, 0)
    kind = (lane // per) % QUAD
    owner = ((kind // 2 + side) % 2) * 2 + (kind % 2 + core) % 2
    want = jnp.zeros(tile, jnp.int32)
    for i in range(per):
        want = jnp.where(lane % per == i, pos_ref[i], want)
    scores, chosen = [], []
    for g in range(G):
        peer_y, peer_z = (y + g // C) % Y, (z + g % C) % C
        ids = ((peer_y * QUAD + owner) * C + peer_z) * per + doc
        tile_scores = sc_in[g]
        scores.append(tile_scores)
        chosen.append(jnp.where(ids == want, tile_scores, 0.0))
    peak = total(jnp.maximum, scores)
    expsum = total(jnp.add, [jnp.exp(t - peak) for t in scores])
    loss = peak + jnp.log(expsum) - total(jnp.add, chosen)
    out_ref[...] = loss[0:1, 0:per]
    for c in started:
        c.wait_send()


def local(Y, C, queries, documents, lengths, positives):
    per, QT, dim = queries.shape
    DT = documents.shape[1]
    G = Y * C
    dma = pltpu.SemaphoreType.DMA
    vmem = pl.BlockSpec(memory_space=pltpu.VMEM)
    smem = pl.BlockSpec(memory_space=pltpu.SMEM)
    out = pl.pallas_call(
        functools.partial(kernel, Y, C, per, QT, DT),
        out_shape=jax.ShapeDtypeStruct((1, per), jnp.float32),
        in_specs=[smem, smem, vmem, vmem],
        out_specs=vmem,
        scratch_shapes=[
            pltpu.VMEM((QUAD, per * DT, dim), jnp.bfloat16),
            pltpu.VMEM((G, per * QT, dim), jnp.bfloat16),
            pltpu.VMEM((G * per, QUAD * per * QT), jnp.float32),
            pltpu.VMEM((QUAD * per * QT, 128), jnp.bfloat16),
            pltpu.VMEM((G, per, 128), jnp.float32),
            pltpu.VMEM((G, per, 128), jnp.float32),
            dma, dma, dma((PARTS,)), dma((PARTS,)), dma((PARTS,)), dma((PARTS,)),
            dma((G,)), dma((G,)), dma((G,)), dma((G,)),
        ],
        compiler_params=pltpu.CompilerParams(collective_id=0, has_side_effects=True),
    )(
        lengths, positives,
        queries.reshape(per * QT, dim), documents.reshape(per * DT, dim),
    )
    return out.reshape(per)


def solution(mesh):
    Y, C = mesh.shape["row"] // QUAD, mesh.shape["col"]
    placed = (
        P(("row", "col"), None, None),
        P(("row", "col"), None, None),
        P(("row", "col")),
        P(("row", "col")),
    )
    return jax.shard_map(
        functools.partial(local, Y, C),
        mesh=mesh, in_specs=placed, out_specs=P(("row", "col")), check_vma=False,
    )
```

```python
import functools

import jax
import jax.numpy as jnp
from jax import lax
from jax.experimental import pallas as pl
from jax.experimental.pallas import tpu as pltpu
from jax.sharding import PartitionSpec as P

MESH = pl.DeviceIdType.MESH
QUAD = 4
PARTS = 4
HALVES = 2


def kernel(
    Y, C, per, QT, DT,
    len_hbm, pos_hbm, q_hbm, d_hbm, out_ref,
    len_ref, pos_ref, d_ref, dbuf, qbuf, best, ones, sc_out, sc_in, in_sem,
    d_send, d_recv, x_send, x_recv, r_send, r_recv, q_send, q_recv, s_send, s_recv,
):
    row, z = lax.axis_index("row"), lax.axis_index("col")
    y, k = row // QUAD, row % QUAD
    core, side = k % 2, k // 2
    core_peer = (row + 1 - 2 * core, z)
    chip_peer = (row + 2 - 4 * side, z)
    G = Y * C
    rows = per * DT
    toks = per * QT
    part = rows // PARTS
    half = toks // HALVES

    def flip(place, d):
        bit, moved = 1, place
        while bit <= d:
            if d & bit:
                moved = moved + bit - 2 * bit * ((place // bit) % 2)
            bit *= 2
        return moved

    def at(dy, dz):
        return (flip(y, dy) * QUAD + k, flip(z, dz))

    def slot(dy, dz):
        return dy * C + dz

    barrier = pltpu.get_barrier_semaphore()
    peers = [core_peer, chip_peer]
    peers += [at(0, d) for d in range(1, C)] + [at(e, 0) for e in range(1, Y)]
    for peer in peers:
        pl.semaphore_signal(barrier, inc=1, device_id=peer, device_id_type=MESH)

    into = [
        pltpu.make_async_copy(len_hbm, len_ref, in_sem.at[0]),
        pltpu.make_async_copy(d_hbm, d_ref, in_sem.at[1]),
        pltpu.make_async_copy(q_hbm, qbuf.at[0], in_sem.at[2]),
        pltpu.make_async_copy(pos_hbm, pos_ref, in_sem.at[3]),
    ]
    for c in into:
        c.start()

    lane = lax.broadcasted_iota(jnp.int32, ones.shape, 1)
    tok = lax.broadcasted_iota(jnp.int32, ones.shape, 0)
    ones[...] = jnp.where(lane % (QUAD * per) == tok // QT, 1.0, 0.0).astype(jnp.bfloat16)

    for c in into:
        c.wait()
    slots = lax.broadcasted_iota(jnp.int32, (DT, d_ref.shape[1]), 0)
    for i in range(per):
        block = d_ref[i * DT:(i + 1) * DT, :].astype(jnp.float32)
        block = jnp.where(slots < len_ref[i], block, block[0:1, :])
        dbuf[0, i * DT:(i + 1) * DT, :] = block.astype(jnp.bfloat16)

    pl.semaphore_wait(barrier, len(peers))

    started = []

    def go(src, dst, send, recv, peer):
        c = pltpu.make_async_remote_copy(
            src_ref=src, dst_ref=dst, send_sem=send, recv_sem=recv,
            device_id=peer, device_id_type=MESH,
        )
        c.start()
        started.append(c)
        return c

    def piece(b, i):
        return dbuf.at[b, pl.ds(i * part, part), :]

    def tokens(s, h):
        return qbuf.at[s, pl.ds(h * half, half), :]

    far = list(range(C - 1, 0, -1))
    got_q = {}

    def send_q(src, s, h, peer):
        got_q[s, h] = go(
            tokens(src, h), tokens(s, h), q_send.at[s, h], q_recv.at[s, h], peer
        )

    for d in far:
        for h in range(HALVES):
            send_q(0, slot(0, d), h, at(0, d))
    for e in range(1, Y):
        for h in range(HALVES):
            send_q(0, slot(e, 0), h, at(e, 0))
    got_x = [
        go(piece(0, i), piece(2, i), x_send.at[i], x_recv.at[i], chip_peer)
        for i in range(PARTS)
    ]
    got_d = go(dbuf.at[0], dbuf.at[1], d_send, d_recv, core_peer)
    got_r = []

    def unit(s, b):
        sim = lax.dot_general(
            dbuf[b], qbuf[s], (((1,), (1,)), ((), ())), preferred_element_type=jnp.float32
        )
        top = jnp.max(sim.reshape(per, DT, toks), axis=1)
        best[s * per:(s + 1) * per, b * toks:(b + 1) * toks] = top

    got_s = []

    def send_scores(s, count):
        x = best[s * per:(s + count) * per, :]
        hi = x.astype(jnp.bfloat16)
        x = x - hi.astype(jnp.float32)
        mid = x.astype(jnp.bfloat16)
        low = (x - mid.astype(jnp.float32)).astype(jnp.bfloat16)
        sums = jnp.dot(low, ones[...], preferred_element_type=jnp.float32)
        sums += jnp.dot(mid, ones[...], preferred_element_type=jnp.float32)
        sums += jnp.dot(hi, ones[...], preferred_element_type=jnp.float32)
        sums = sums.reshape(count, per, sums.shape[1])
        for i in range(count):
            if s + i == 0:
                sc_in[0] = sums[0]
            else:
                sc_out[s + i] = sums[i]
        for i in range(count - 1, -1, -1):
            t = s + i
            if t:
                got_s.append(go(
                    sc_out.at[t], sc_in.at[t], s_send.at[t], s_recv.at[t], at(t // C, t % C)
                ))

    unit(0, 0)
    got_d.wait_recv()
    unit(0, 1)
    for i in range(max(PARTS, C - 1)):
        if i < C - 1:
            s = slot(0, far[i])
            for h in range(HALVES):
                got_q[s, h].wait_recv()
                for e in range(1, Y):
                    send_q(s, slot(e, far[i]), h, at(e, 0))
        if i < PARTS:
            got_x[i].wait_recv()
            got_r.append(
                go(piece(2, i), piece(3, i), r_send.at[i], r_recv.at[i], core_peer)
            )
        if i < C - 1:
            unit(s, 0)
            unit(s, 1)
    for e in range(1, Y):
        s = slot(e, 0)
        for h in range(HALVES):
            got_q[s, h].wait_recv()
        unit(s, 0)
        unit(s, 1)
    near = [slot(0, d) for d in range(C)] + [slot(e, 0) for e in range(1, Y)]
    for s in near:
        unit(s, 2)
    for c in got_r:
        c.wait_recv()
    for s in near:
        unit(s, 3)
    send_scores(0, C)
    for e in range(1, Y):
        send_scores(slot(e, 0), 1)
    for d in far:
        for e in range(1, Y):
            s = slot(e, d)
            for h in range(HALVES):
                got_q[s, h].wait_recv()
            for b in range(QUAD):
                unit(s, b)
            send_scores(s, 1)

    def total(op, tiles):
        t = tiles[0]
        for g in range(1, G):
            t = op(t, tiles[g])
        shift = 1
        while shift < per:
            t = op(t, pltpu.roll(t, shift, 0))
            shift *= 2
        shift = per
        while shift < QUAD * per:
            t = op(t, pltpu.roll(t, shift, 1))
            shift *= 2
        return t

    tile = sc_in.shape[1:]
    lane = lax.broadcasted_iota(jnp.int32, tile, 1)
    doc = lax.broadcasted_iota(jnp.int32, tile, 0)
    kind = (lane // per) % QUAD
    owner = ((kind // 2 + side) % 2) * 2 + (kind % 2 + core) % 2
    want = jnp.zeros(tile, jnp.int32)
    for i in range(per):
        want = jnp.where(lane % per == i, pos_ref[i], want)
    for c in got_s:
        c.wait_recv()
    scores, chosen = [], []
    for g in range(G):
        ids = ((flip(y, g // C) * QUAD + owner) * C + flip(z, g % C)) * per + doc
        tile_scores = sc_in[g]
        scores.append(tile_scores)
        chosen.append(jnp.where(ids == want, tile_scores, 0.0))
    peak = total(jnp.maximum, scores)
    expsum = total(jnp.add, [jnp.exp(t - peak) for t in scores])
    loss = peak + jnp.log(expsum) - total(jnp.add, chosen)
    out_ref[...] = loss[0:1, 0:per].reshape(per)
    for c in started:
        c.wait_send()


def local(Y, C, queries, documents, lengths, positives):
    per, QT, dim = queries.shape
    DT = documents.shape[1]
    G = Y * C
    dma = pltpu.SemaphoreType.DMA
    anywhere = pl.BlockSpec(memory_space=pl.ANY)
    return pl.pallas_call(
        functools.partial(kernel, Y, C, per, QT, DT),
        out_shape=jax.ShapeDtypeStruct((per,), jnp.float32),
        in_specs=[anywhere] * 4,
        out_specs=pl.BlockSpec(memory_space=pltpu.VMEM),
        scratch_shapes=[
            pltpu.SMEM((per,), jnp.int32),
            pltpu.SMEM((per,), jnp.int32),
            pltpu.VMEM((per * DT, dim), jnp.bfloat16),
            pltpu.VMEM((QUAD, per * DT, dim), jnp.bfloat16),
            pltpu.VMEM((G, per * QT, dim), jnp.bfloat16),
            pltpu.VMEM((G * per, QUAD * per * QT), jnp.float32),
            pltpu.VMEM((QUAD * per * QT, 128), jnp.bfloat16),
            pltpu.VMEM((G, per, 128), jnp.float32),
            pltpu.VMEM((G, per, 128), jnp.float32),
            dma((4,)),
            dma, dma, dma((PARTS,)), dma((PARTS,)), dma((PARTS,)), dma((PARTS,)),
            dma((G, HALVES)), dma((G, HALVES)), dma((G,)), dma((G,)),
        ],
        compiler_params=pltpu.CompilerParams(collective_id=0, has_side_effects=True),
    )(
        lengths, positives,
        queries.reshape(per * QT, dim), documents.reshape(per * DT, dim),
    )


def solution(mesh):
    Y, C = mesh.shape["row"] // QUAD, mesh.shape["col"]
    placed = (
        P(("row", "col"), None, None),
        P(("row", "col"), None, None),
        P(("row", "col")),
        P(("row", "col")),
    )
    return jax.shard_map(
        functools.partial(local, Y, C),
        mesh=mesh, in_specs=placed, out_specs=P(("row", "col")), check_vma=False,
    )
```

```python
import functools

import jax
import jax.numpy as jnp
from jax import lax
from jax.experimental import pallas as pl
from jax.experimental.pallas import tpu as pltpu
from jax.sharding import PartitionSpec as P

MESH = pl.DeviceIdType.MESH
QUAD = 4
PARTS = 4
HALVES = 2


def kernel(
    Y, C, per, QT, DT,
    len_hbm, pos_hbm, q_hbm, d_hbm, out_ref,
    len_ref, pos_ref, d_ref, dbuf, qbuf, best, ones, sc_out, sc_in, in_sem,
    d_send, d_recv, x_send, x_recv, r_send, r_recv, q_send, q_recv, s_send, s_recv,
):
    row, z = lax.axis_index("row"), lax.axis_index("col")
    y, k = row // QUAD, row % QUAD
    core, side = k % 2, k // 2
    core_peer = (row + 1 - 2 * core, z)
    chip_peer = (row + 2 - 4 * side, z)
    G = Y * C
    rows = per * DT
    toks = per * QT
    part = rows // PARTS
    half = toks // HALVES

    def flip(place, d):
        bit, moved = 1, place
        while bit <= d:
            if d & bit:
                moved = moved + bit - 2 * bit * ((place // bit) % 2)
            bit *= 2
        return moved

    def at(dy, dz):
        return (flip(y, dy) * QUAD + k, flip(z, dz))

    def slot(dy, dz):
        return dy * C + dz

    barrier = pltpu.get_barrier_semaphore()
    peers = [core_peer, chip_peer]
    peers += [at(0, d) for d in range(1, C)] + [at(e, 0) for e in range(1, Y)]
    for peer in peers:
        pl.semaphore_signal(barrier, inc=1, device_id=peer, device_id_type=MESH)

    into = [
        pltpu.make_async_copy(len_hbm, len_ref, in_sem.at[0]),
        pltpu.make_async_copy(d_hbm, d_ref, in_sem.at[1]),
        pltpu.make_async_copy(q_hbm, qbuf.at[0], in_sem.at[2]),
        pltpu.make_async_copy(pos_hbm, pos_ref, in_sem.at[3]),
    ]
    for c in into:
        c.start()

    lane = lax.broadcasted_iota(jnp.int32, ones.shape, 1)
    tok = lax.broadcasted_iota(jnp.int32, ones.shape, 0)
    ones[...] = jnp.where(lane % (QUAD * per) == tok // QT, 1.0, 0.0).astype(jnp.bfloat16)

    for c in into:
        c.wait()
    slots = lax.broadcasted_iota(jnp.int32, (DT, d_ref.shape[1]), 0)
    for i in range(per):
        block = d_ref[i * DT:(i + 1) * DT, :].astype(jnp.float32)
        block = jnp.where(slots < len_ref[i], block, block[0:1, :])
        dbuf[0, i * DT:(i + 1) * DT, :] = block.astype(jnp.bfloat16)

    pl.semaphore_wait(barrier, len(peers))

    started = []

    def go(src, dst, send, recv, peer):
        c = pltpu.make_async_remote_copy(
            src_ref=src, dst_ref=dst, send_sem=send, recv_sem=recv,
            device_id=peer, device_id_type=MESH,
        )
        c.start()
        started.append(c)
        return c

    def piece(b, i):
        return dbuf.at[b, pl.ds(i * part, part), :]

    def tokens(s, h):
        return qbuf.at[s, pl.ds(h * half, half), :]

    far = list(range(C - 1, 0, -1))
    got_q = {}

    def send_q(src, s, h, peer):
        got_q[s, h] = go(
            tokens(src, h), tokens(s, h), q_send.at[s, h], q_recv.at[s, h], peer
        )

    for d in far:
        for h in range(HALVES):
            send_q(0, slot(0, d), h, at(0, d))
    for e in range(1, Y):
        for h in range(HALVES):
            send_q(0, slot(e, 0), h, at(e, 0))
    got_x = [
        go(piece(0, i), piece(2, i), x_send.at[i], x_recv.at[i], chip_peer)
        for i in range(PARTS)
    ]
    got_d = go(dbuf.at[0], dbuf.at[1], d_send, d_recv, core_peer)
    got_r = []

    def unit(s, b):
        sim = lax.dot_general(
            dbuf[b], qbuf[s], (((1,), (1,)), ((), ())), preferred_element_type=jnp.float32
        )
        top = jnp.max(sim.reshape(per, DT, toks), axis=1)
        best[s * per:(s + 1) * per, b * toks:(b + 1) * toks] = top

    got_s = []

    def send_scores(s, count):
        x = best[s * per:(s + count) * per, :]
        hi = x.astype(jnp.bfloat16)
        x = x - hi.astype(jnp.float32)
        mid = x.astype(jnp.bfloat16)
        low = (x - mid.astype(jnp.float32)).astype(jnp.bfloat16)
        sums = jnp.dot(low, ones[...], preferred_element_type=jnp.float32)
        sums += jnp.dot(mid, ones[...], preferred_element_type=jnp.float32)
        sums += jnp.dot(hi, ones[...], preferred_element_type=jnp.float32)
        sums = sums.reshape(count, per, sums.shape[1])
        for i in range(count):
            if s + i == 0:
                sc_in[0] = sums[0]
            else:
                sc_out[s + i] = sums[i]
        for i in range(count - 1, -1, -1):
            t = s + i
            if t:
                got_s.append(go(
                    sc_out.at[t], sc_in.at[t], s_send.at[t], s_recv.at[t], at(t // C, t % C)
                ))

    unit(0, 0)
    got_d.wait_recv()
    unit(0, 1)
    for e in range(1, Y):
        s = slot(e, 0)
        for h in range(HALVES):
            got_q[s, h].wait_recv()
        unit(s, 0)
        unit(s, 1)
    for i in range(max(PARTS, C - 1)):
        if i < C - 1:
            s = slot(0, far[i])
            for h in range(HALVES):
                got_q[s, h].wait_recv()
                for e in range(1, Y):
                    send_q(s, slot(e, far[i]), h, at(e, 0))
        if i < PARTS:
            got_x[i].wait_recv()
            got_r.append(
                go(piece(2, i), piece(3, i), r_send.at[i], r_recv.at[i], core_peer)
            )
        if i < C - 1:
            unit(s, 0)
            unit(s, 1)
    near = [slot(0, d) for d in range(C)] + [slot(e, 0) for e in range(1, Y)]
    for s in near:
        unit(s, 2)
    for c in got_r:
        c.wait_recv()
    for s in near:
        unit(s, 3)
    send_scores(0, C)
    for e in range(1, Y):
        send_scores(slot(e, 0), 1)
    for d in far:
        for e in range(1, Y):
            s = slot(e, d)
            for h in range(HALVES):
                got_q[s, h].wait_recv()
            for b in range(QUAD):
                unit(s, b)
            send_scores(s, 1)

    def total(op, tiles):
        t = tiles[0]
        for g in range(1, G):
            t = op(t, tiles[g])
        shift = 1
        while shift < per:
            t = op(t, pltpu.roll(t, shift, 0))
            shift *= 2
        shift = per
        while shift < QUAD * per:
            t = op(t, pltpu.roll(t, shift, 1))
            shift *= 2
        return t

    tile = sc_in.shape[1:]
    lane = lax.broadcasted_iota(jnp.int32, tile, 1)
    doc = lax.broadcasted_iota(jnp.int32, tile, 0)
    kind = (lane // per) % QUAD
    owner = ((kind // 2 + side) % 2) * 2 + (kind % 2 + core) % 2
    want = jnp.zeros(tile, jnp.int32)
    for i in range(per):
        want = jnp.where(lane % per == i, pos_ref[i], want)
    for c in got_s:
        c.wait_recv()
    scores, chosen = [], []
    for g in range(G):
        ids = ((flip(y, g // C) * QUAD + owner) * C + flip(z, g % C)) * per + doc
        tile_scores = sc_in[g]
        scores.append(tile_scores)
        chosen.append(jnp.where(ids == want, tile_scores, 0.0))
    peak = total(jnp.maximum, scores)
    expsum = total(jnp.add, [jnp.exp(t - peak) for t in scores])
    loss = peak + jnp.log(expsum) - total(jnp.add, chosen)
    out_ref[...] = loss[0:1, 0:per].reshape(per)
    for c in started:
        c.wait_send()


def local(Y, C, queries, documents, lengths, positives):
    per, QT, dim = queries.shape
    DT = documents.shape[1]
    G = Y * C
    dma = pltpu.SemaphoreType.DMA
    anywhere = pl.BlockSpec(memory_space=pl.ANY)
    return pl.pallas_call(
        functools.partial(kernel, Y, C, per, QT, DT),
        out_shape=jax.ShapeDtypeStruct((per,), jnp.float32),
        in_specs=[anywhere] * 4,
        out_specs=pl.BlockSpec(memory_space=pltpu.VMEM),
        scratch_shapes=[
            pltpu.SMEM((per,), jnp.int32),
            pltpu.SMEM((per,), jnp.int32),
            pltpu.VMEM((per * DT, dim), jnp.bfloat16),
            pltpu.VMEM((QUAD, per * DT, dim), jnp.bfloat16),
            pltpu.VMEM((G, per * QT, dim), jnp.bfloat16),
            pltpu.VMEM((G * per, QUAD * per * QT), jnp.float32),
            pltpu.VMEM((QUAD * per * QT, 128), jnp.bfloat16),
            pltpu.VMEM((G, per, 128), jnp.float32),
            pltpu.VMEM((G, per, 128), jnp.float32),
            dma((4,)),
            dma, dma, dma((PARTS,)), dma((PARTS,)), dma((PARTS,)), dma((PARTS,)),
            dma((G, HALVES)), dma((G, HALVES)), dma((G,)), dma((G,)),
        ],
        compiler_params=pltpu.CompilerParams(collective_id=0, has_side_effects=True),
    )(
        lengths, positives,
        queries.reshape(per * QT, dim), documents.reshape(per * DT, dim),
    )


def solution(mesh):
    Y, C = mesh.shape["row"] // QUAD, mesh.shape["col"]
    placed = (
        P(("row", "col"), None, None),
        P(("row", "col"), None, None),
        P(("row", "col")),
        P(("row", "col")),
    )
    return jax.shard_map(
        functools.partial(local, Y, C),
        mesh=mesh, in_specs=placed, out_specs=P(("row", "col")), check_vma=False,
    )
```
